32 devices in a mesh: dp: 2 (over core), tensor: 16 (over z, y, x).
Axes of the slice: x: 2, y: 2, z: 4, core: 2. Of those that a mesh axis runs over, the one named last changes fastest.
Arguments:
- inputs: bfloat16 [768, 6144], P(('dp', 'tensor')), may hold values from -0.29882812 to 0.29882812
- norm_gain: float32 [6144], replicated, may hold values from 0.1 to 1.9
- norm_bias: float32 [6144], replicated, may hold values from -3 to 3
- query_grad: bfloat16 [768, 12288], P('dp', 'tensor'), may hold values from -0.119628906 to 0.119628906
- stream_grad: bfloat16 [768, 6144], P(('dp', 'tensor')), may hold values from -2.390625 to 2.390625
- query_weight: bfloat16 [6144, 12288], P(None, 'tensor'), may hold values from -0.0546875 to 0.0546875
Outputs:
- input_grad: bfloat16 [768, 6144], P(('dp', 'tensor'))
- weight_grad: bfloat16 [6144, 12288], P(None, 'tensor')
The draws below stay inside these ranges and needn't reach their ends.
All inputs are finite; a program needn't handle non-finite values.
Results may differ from the reference program's by a relative error of at most 0.019.
Values may be sent and summed in bfloat16 or wider, within the bound.
No kernel may reach another device: no remote copies, remote signals or barrier semaphores. Data moves between devices by JAX's collectives and lax.ppermute only.
A program may use at most 128 MiB of HBM per device.

```python
import jax
import jax.numpy as jnp
from jax import lax

D = 6144
HEADS = 96
HD = 128
TOK_DEV = 24
TOKENS = 768
COLUMNS = 12288
N_DP = 2
N_TENSOR = 16


def strengthened(values, own_key, source, target, blocks, factor):
    owner, partner = [(jnp.arange(values.shape[axis_at]) // (values.shape[axis_at] // blocks)).reshape([-1 if axis == axis_at else 1 for axis in range(values.ndim)]) for axis_at in (source, target)]
    chosen = jax.random.permutation(own_key, blocks)[partner]
    strong = (owner == chosen) | (owner == (partner + blocks // 2) % blocks)
    return jnp.where(strong, factor * values, values)


def steps_of(rng, dims, cuts, low, high):
    def one(dim, shards_of):
        draws = jax.random.uniform(jax.random.fold_in(jax.random.fold_in(rng, 6), dim), (shards_of,), jnp.float32, low / len(cuts), high / len(cuts))
        return jnp.repeat(jnp.exp(draws), dims[dim] // shards_of).reshape((-1,) + (1,) * (len(dims) - dim - 1))

    factor_of = one(*cuts[0])
    for cut in cuts[1:]:
        factor_of = factor_of * one(*cut)
    return factor_of


def centred(own_key, shape, width, limit, cuts=(), kind=jnp.bfloat16):
    entries = jax.random.normal(own_key, shape, jnp.float32) * width
    if len(cuts) > 0:
        entries = steps_of(own_key, shape, cuts, -0.22, 0.18) * entries
    return jnp.clip(entries, min=-limit, max=limit).astype(kind)


def heavy_noise(stream_key, extent, scale, most, cuts, heavy, held_as=jnp.bfloat16):
    values = scale * jax.random.normal(stream_key, extent, jnp.float32)
    if cuts:
        values = values * steps_of(stream_key, extent, cuts, -0.22, 0.18)
    return jnp.clip(strengthened(values, jax.random.fold_in(stream_key, 3), *heavy), -most, most).astype(held_as)


def setup_inputs(seed: int = 0) -> dict:
    key_list = jax.random.split(jax.random.key(seed), 7)
    inputs = centred(key_list[0], (TOKENS, D), 0.05, 0.29882812, ((0, 32),))
    norm_gain = jnp.clip(1.0 + 0.18 * jax.random.normal(key_list[1], (D,), jnp.float32), 0.1, 1.9)
    norm_bias = centred(key_list[2], (D,), 0.5, 3.0, (), jnp.float32)
    query_grad = heavy_noise(key_list[3], (TOKENS, COLUMNS), 0.02, 0.119628906, ((0, 2), (1, 16)), (1, 0, 16, 2.0))
    stream_grad = centred(key_list[4], (TOKENS, D), 0.4, 2.390625, ((0, 32),))
    query_weight = centred(key_list[5], (D, COLUMNS), COLUMNS ** -0.5, 0.0546875, ((1, 16),))
    return {"inputs": inputs, "norm_gain": norm_gain, "norm_bias": norm_bias, "query_grad": query_grad, "stream_grad": stream_grad, "query_weight": query_weight}


epsilon = 1e-05

def normalize(values, norm_gain, norm_bias):
    as_float = values.astype(jnp.float32)
    centre = lax.optimization_barrier(jnp.mean(as_float, axis=-1, keepdims=True))
    offsets = as_float - centre
    variance = lax.optimization_barrier(jnp.mean(offsets * offsets, axis=-1, keepdims=True))
    inverse = lax.rsqrt(variance + epsilon)
    scaled = offsets * inverse
    normed = (scaled * norm_gain + norm_bias).astype(jnp.bfloat16)
    return (scaled, inverse, normed)

def norm_backward(scaled, inverse, normed_grad, norm_gain, stream_grad):
    weighted = normed_grad * norm_gain
    first_moment = lax.optimization_barrier(jnp.mean(weighted, axis=-1, keepdims=True))
    second_moment = lax.optimization_barrier(jnp.mean(weighted * scaled, axis=-1, keepdims=True))
    result = stream_grad.astype(jnp.float32) + inverse * (weighted - first_moment - scaled * second_moment)
    return result.astype(jnp.bfloat16)

def reference(inputs, norm_gain, norm_bias, query_grad, stream_grad, query_weight):
    per_group = TOK_DEV * N_TENSOR
    columns = HEADS * HD
    width_dev = columns // N_TENSOR
    grouped_in = inputs.reshape(N_DP, per_group, D)
    grouped_grad = query_grad.reshape(N_DP, per_group, columns)
    grouped_stream = stream_grad.reshape(N_DP, per_group, D)

    def group_step(carried, items):
        rows_in, rows_grad, rows_stream = items
        scaled, inverse, normed = normalize(rows_in, norm_gain, norm_bias)
        partial_value = jnp.dot(normed.T, rows_grad, preferred_element_type=jnp.float32)
        rounded = lax.optimization_barrier(partial_value.astype(jnp.bfloat16)).astype(jnp.float32)

        def add_block(running, block):
            begin = (block * width_dev).astype(jnp.int32)
            grad_cols = lax.dynamic_slice_in_dim(rows_grad, begin, width_dev, 1)
            weight_cols = lax.dynamic_slice_in_dim(query_weight, begin, width_dev, 1)
            term = lax.dot_general(grad_cols, weight_cols, (((1,), (1,)), ((), ())), preferred_element_type=jnp.float32)
            return (running + lax.optimization_barrier(term.astype(jnp.bfloat16)).astype(jnp.float32), None)
        normed_grad, _ = lax.scan(add_block, jnp.zeros((per_group, D), jnp.float32), jnp.arange(N_TENSOR, dtype=jnp.int32))
        grads_out = norm_backward(scaled, inverse, normed_grad, norm_gain, rows_stream)
        return (carried + rounded, grads_out)
    weight_grad, input_grad = lax.scan(group_step, jnp.zeros((D, columns), jnp.float32), (grouped_in, grouped_grad, grouped_stream))
    return (input_grad.reshape(N_DP * per_group, D), weight_grad.astype(jnp.bfloat16))
```

```python
import jax
import jax.numpy as jnp
from jax import lax
from jax.experimental import pallas as pl
from jax.experimental.pallas import tpu as pltpu
from jax.sharding import PartitionSpec as P

epsilon = 1e-05


def sizes_of(count):
    outer = 4 if count % 4 == 0 else 1
    rest = count // outer
    inner = 2 if rest % 2 == 0 else 1
    return (outer, rest // inner, inner)


def moved(sizes, axis, step):
    outer, middle, inner = sizes
    pairs = []
    for index in range(outer * middle * inner):
        place = [index // (middle * inner), index // inner % middle, index % inner]
        place[axis] = (place[axis] + step) % sizes[axis]
        pairs.append((index, (place[0] * middle + place[1]) * inner + place[2]))
    return pairs


def gather_pieces(sizes, axis, values):
    return [values] + [
        lax.ppermute(values, "tensor", moved(sizes, axis, -step)) for step in range(1, sizes[axis])
    ]


def row_selector(sizes, order, rows):
    index = lax.axis_index("tensor")
    outer, middle, inner = sizes
    own = [index // (middle * inner), index // inner % middle, index % inner]
    count = outer * middle * inner
    tokens = rows // count
    row = lax.broadcasted_iota(jnp.int32, (rows, rows), 0)
    column = lax.broadcasted_iota(jnp.int32, (rows, rows), 1)
    left = row // tokens
    places = [None, None, None]
    for axis in reversed(order):
        places[axis] = (left % sizes[axis] + own[axis]) % sizes[axis]
        left = left // sizes[axis]
    source = ((places[0] * middle + places[1]) * inner + places[2]) * tokens + row % tokens
    return (source == column).astype(jnp.bfloat16)


def picked(selector, values):
    return lax.dot_general(
        selector, values, (((1,), (0,)), ((), ())), preferred_element_type=jnp.float32
    ).astype(jnp.bfloat16)


def weight_kernel(halves, steps_half):
    counts = [len(half) for half in halves]

    def body(*refs):
        out_ref = refs[-1]
        ins = refs[:-1]
        step = pl.program_id(0)
        start = 0
        for number, count in enumerate(counts):
            piece_refs = ins[start : start + count]
            grad_ref = ins[start + count]
            start += count + 1

            @pl.when(step // steps_half == number)
            def _():
                total = None
                at = 0
                for piece_ref in piece_refs:
                    rows = piece_ref.shape[0]
                    part = lax.dot_general(
                        piece_ref[...],
                        grad_ref[at : at + rows, :],
                        (((0,), (0,)), ((), ())),
                        preferred_element_type=jnp.float32,
                    )
                    at += rows
                    total = part if total is None else total + part
                out_ref[...] = total.astype(out_ref.dtype)

    return body


def weight_product(halves, grads):
    width = halves[0][0].shape[1]
    block = next(size for size in (512, 256, 128) if width % size == 0)
    steps_half = width // block
    features = grads[0].shape[1]
    specs, operands = [], []
    for number, (pieces, grad) in enumerate(zip(halves, grads)):
        for piece in pieces:
            specs.append(
                pl.BlockSpec(
                    (piece.shape[0], block),
                    lambda i, n=number: (0, jnp.clip(i - n * steps_half, 0, steps_half - 1)),
                )
            )
            operands.append(piece)
        specs.append(pl.BlockSpec(grad.shape, lambda i: (0, 0)))
        operands.append(grad)
    rows = grads[0].shape[0]
    return pl.pallas_call(
        weight_kernel(halves, steps_half),
        grid=(2 * steps_half,),
        in_specs=specs,
        out_specs=pl.BlockSpec((block, features), lambda i: (i, 0)),
        out_shape=jax.ShapeDtypeStruct((2 * width, features), jnp.bfloat16),
        cost_estimate=pl.CostEstimate(
            flops=4 * rows * width * features, transcendentals=0, bytes_accessed=4 * width * features
        ),
        name="weight_product",
    )(*operands)


def normalize(values, norm_gain, norm_bias):
    as_float = values.astype(jnp.float32)
    centre = jnp.mean(as_float, axis=-1, keepdims=True)
    offsets = as_float - centre
    variance = jnp.mean(offsets * offsets, axis=-1, keepdims=True)
    inverse = lax.rsqrt(variance + epsilon)
    scaled = offsets * inverse
    normed = (scaled * norm_gain + norm_bias).astype(jnp.bfloat16)
    return (scaled, inverse, normed)


def norm_backward(scaled, inverse, normed_grad, norm_gain, stream_grad):
    weighted = normed_grad * norm_gain
    first_moment = jnp.mean(weighted, axis=-1, keepdims=True)
    second_moment = jnp.mean(weighted * scaled, axis=-1, keepdims=True)
    result = stream_grad.astype(jnp.float32) + inverse * (
        weighted - first_moment - scaled * second_moment
    )
    return result.astype(jnp.bfloat16)


def summed(values, sizes, axis):
    rows = values[0].shape[0]
    total = values[0].astype(jnp.float32)
    for step in range(1, sizes[axis]):
        total = total + lax.ppermute(values[step], "tensor", moved(sizes, axis, step)).astype(
            jnp.float32
        )
    return total


def program(sizes, groups):
    orders = ((2, 1, 0), (1, 2, 0))

    def shards(inputs, norm_gain, norm_bias, query_grad, stream_grad, query_weight):
        width = inputs.shape[1] // 2
        rows = query_grad.shape[0]
        paired = groups == 2
        swap = [(0, 1), (1, 0)]

        scaled, inverse, normed = normalize(inputs, norm_gain, norm_bias)
        outer_pieces = gather_pieces(sizes, 0, normed)
        other_grad = lax.ppermute(query_grad, "dp", swap) if paired else None
        selectors = [row_selector(sizes, order, rows) for order in orders]
        grads = [picked(selector, query_grad) for selector in selectors]

        chunks = []
        for number, order in enumerate(orders):
            count = sizes[order[0]]
            tall = rows // count
            weight_rows = query_weight[number * width : (number + 1) * width]
            made = [
                lax.dot_general(
                    grads[number][step * tall : (step + 1) * tall],
                    weight_rows,
                    (((1,), (1,)), ((), ())),
                    preferred_element_type=jnp.float32,
                ).astype(jnp.bfloat16)
                for step in range(count)
            ]
            chunks.append(made)
        ends = []
        for number, order in enumerate(orders):
            total = summed(chunks[number], sizes, order[0]).astype(jnp.bfloat16)
            count = sizes[order[1]]
            tall = total.shape[0] // count
            total = summed(
                [total[step * tall : (step + 1) * tall] for step in range(count)], sizes, order[1]
            ).astype(jnp.bfloat16)
            count = sizes[0]
            tall = total.shape[0] // count
            ends.append(
                summed([total[step * tall : (step + 1) * tall] for step in range(count)], sizes, 0)
            )
        normed_grad = jnp.concatenate(ends, axis=1)
        input_grad = norm_backward(scaled, inverse, normed_grad, norm_gain, stream_grad)

        halves = []
        for number, order in enumerate(orders):
            held = jnp.concatenate(
                [piece[:, number * width : (number + 1) * width] for piece in outer_pieces], axis=0
            )
            held = jnp.concatenate(gather_pieces(sizes, order[1], held), axis=0)
            pieces = gather_pieces(sizes, order[0], held)
            if paired:
                pieces = pieces + [lax.ppermute(piece, "dp", swap) for piece in pieces]
            halves.append(pieces)
        if paired:
            grads = [
                jnp.concatenate([grad, picked(selector, other_grad)], axis=0)
                for grad, selector in zip(grads, selectors)
            ]
        weight_grad = weight_product(halves, grads)
        if groups > 1 and not paired:
            weight_grad = lax.psum(weight_grad, "dp")
        return (input_grad, weight_grad)

    return shards


def solution(mesh):
    placed = (
        P(("dp", "tensor"), None),
        P(),
        P(),
        P("dp", "tensor"),
        P(("dp", "tensor"), None),
        P(None, "tensor"),
    )
    return jax.shard_map(
        program(sizes_of(mesh.shape["tensor"]), mesh.shape["dp"]),
        mesh=mesh,
        in_specs=placed,
        out_specs=(P(("dp", "tensor"), None), P(None, "tensor")),
        check_vma=False,
    )
```

```python
import jax
import jax.numpy as jnp
from jax import lax
from jax.experimental import pallas as pl
from jax.sharding import PartitionSpec as P

epsilon = 1e-05


def sizes_of(count):
    outer = 4 if count % 4 == 0 else 1
    rest = count // outer
    inner = 2 if rest % 2 == 0 else 1
    return (outer, rest // inner, inner)


def moved(sizes, axis, step):
    outer, middle, inner = sizes
    pairs = []
    for index in range(outer * middle * inner):
        place = [index // (middle * inner), index // inner % middle, index % inner]
        place[axis] = (place[axis] + step) % sizes[axis]
        pairs.append((index, (place[0] * middle + place[1]) * inner + place[2]))
    return pairs


def gather_pieces(sizes, axis, values):
    return [values] + [
        lax.ppermute(values, "tensor", moved(sizes, axis, -step)) for step in range(1, sizes[axis])
    ]


def row_selector(sizes, order, rows):
    index = lax.axis_index("tensor")
    outer, middle, inner = sizes
    own = [index // (middle * inner), index // inner % middle, index % inner]
    count = outer * middle * inner
    tokens = rows // count
    row = lax.broadcasted_iota(jnp.int32, (rows, rows), 0)
    column = lax.broadcasted_iota(jnp.int32, (rows, rows), 1)
    left = row // tokens
    places = [None, None, None]
    for axis in reversed(order):
        places[axis] = (left % sizes[axis] + own[axis]) % sizes[axis]
        left = left // sizes[axis]
    source = ((places[0] * middle + places[1]) * inner + places[2]) * tokens + row % tokens
    return (source == column).astype(jnp.bfloat16)


def picked(selector, values):
    return lax.dot_general(
        selector, values, (((1,), (0,)), ((), ())), preferred_element_type=jnp.float32
    ).astype(jnp.bfloat16)


def weight_kernel(halves, steps_half):
    counts = [len(half) for half in halves]

    def body(*refs):
        out_ref = refs[-1]
        ins = refs[:-1]
        step = pl.program_id(0)
        start = 0
        for number, count in enumerate(counts):
            piece_refs = ins[start : start + count]
            grad_ref = ins[start + count]
            start += count + 1

            @pl.when(step // steps_half == number)
            def _():
                tall = jnp.concatenate([ref[...] for ref in piece_refs], axis=0)
                out_ref[...] = lax.dot_general(
                    tall, grad_ref[...], (((0,), (0,)), ((), ())), preferred_element_type=jnp.float32
                ).astype(out_ref.dtype)

    return body


def weight_product(halves, grads):
    width = halves[0][0].shape[1]
    block = next(size for size in (512, 256, 128) if width % size == 0)
    steps_half = width // block
    features = grads[0].shape[1]
    specs, operands = [], []
    for number, (pieces, grad) in enumerate(zip(halves, grads)):
        for piece in pieces:
            specs.append(
                pl.BlockSpec(
                    (piece.shape[0], block),
                    lambda i, n=number: (0, jnp.clip(i - n * steps_half, 0, steps_half - 1)),
                )
            )
            operands.append(piece)
        specs.append(pl.BlockSpec(grad.shape, lambda i: (0, 0)))
        operands.append(grad)
    rows = grads[0].shape[0]
    return pl.pallas_call(
        weight_kernel(halves, steps_half),
        grid=(2 * steps_half,),
        in_specs=specs,
        out_specs=pl.BlockSpec((block, features), lambda i: (i, 0)),
        out_shape=jax.ShapeDtypeStruct((2 * width, features), jnp.bfloat16),
        cost_estimate=pl.CostEstimate(
            flops=4 * rows * width * features, transcendentals=0, bytes_accessed=4 * width * features
        ),
        name="weight_product",
    )(*operands)


def after(value, *others):
    return lax.optimization_barrier((value,) + others)[0]


def normalize(values, norm_gain, norm_bias):
    as_float = values.astype(jnp.float32)
    centre = jnp.mean(as_float, axis=-1, keepdims=True)
    offsets = as_float - centre
    variance = jnp.mean(offsets * offsets, axis=-1, keepdims=True)
    inverse = lax.rsqrt(variance + epsilon)
    scaled = offsets * inverse
    normed = (scaled * norm_gain + norm_bias).astype(jnp.bfloat16)
    return (scaled, inverse, normed)


def norm_backward(scaled, inverse, normed_grad, norm_gain, stream_grad):
    weighted = normed_grad * norm_gain
    first_moment = jnp.mean(weighted, axis=-1, keepdims=True)
    second_moment = jnp.mean(weighted * scaled, axis=-1, keepdims=True)
    result = stream_grad.astype(jnp.float32) + inverse * (
        weighted - first_moment - scaled * second_moment
    )
    return result.astype(jnp.bfloat16)


def split(values, count):
    tall = values.shape[0] // count
    return [values[step * tall : (step + 1) * tall] for step in range(count)]


def sent(chunks, sizes, axis):
    return [
        lax.ppermute(chunks[step], "tensor", moved(sizes, axis, step))
        for step in range(1, sizes[axis])
    ]


def added(own, received):
    total = own.astype(jnp.float32)
    for values in received:
        total = total + values.astype(jnp.float32)
    return total


def contracted(grad, weight_rows):
    return lax.dot_general(
        grad, weight_rows, (((1,), (1,)), ((), ())), preferred_element_type=jnp.float32
    ).astype(jnp.bfloat16)


def program(sizes, groups):
    orders = ((2, 1, 0), (1, 2, 0))

    def shards(inputs, norm_gain, norm_bias, query_grad, stream_grad, query_weight):
        width = inputs.shape[1] // 2
        rows = query_grad.shape[0]
        paired = groups == 2
        swap = [(0, 1), (1, 0)]

        scaled, inverse, normed = normalize(inputs, norm_gain, norm_bias)
        normed = after(normed)
        outer_pieces = gather_pieces(sizes, 0, normed)
        query_grad = after(query_grad, normed)
        other_grad = lax.ppermute(query_grad, "dp", swap) if paired else None
        selectors = [row_selector(sizes, order, rows) for order in orders]
        grads = [picked(selector, query_grad) for selector in selectors]

        leaving, kept = [], []
        for number, order in enumerate(orders):
            weight_rows = query_weight[number * width : (number + 1) * width]
            made = [contracted(grad, weight_rows) for grad in split(grads[number], sizes[order[0]])]
            leaving.append(sent(made, sizes, order[0]))
            kept.append(made[0])
        if paired:
            other = [picked(selector, other_grad) for selector in selectors]
            grads = [jnp.concatenate(pair, axis=0) for pair in zip(grads, other)]

        held = [
            jnp.concatenate(
                [piece[:, number * width : (number + 1) * width] for piece in outer_pieces], axis=0
            )
            for number in range(2)
        ]
        *held, kept[0], kept[1] = lax.optimization_barrier((*held, *kept))
        second = [gather_pieces(sizes, order[1], held[n]) for n, order in enumerate(orders)]

        totals = [
            added(kept[n], leaving[n]).astype(jnp.bfloat16) for n in range(2)
        ]
        chunks = [split(totals[n], sizes[order[1]]) for n, order in enumerate(orders)]
        received = [sent(chunks[n], sizes, order[1]) for n, order in enumerate(orders)]

        held = [jnp.concatenate(pieces, axis=0) for pieces in second]
        kept = [chunk[0] for chunk in chunks]
        *held, kept[0], kept[1] = lax.optimization_barrier((*held, *kept, *grads))[:4]
        halves = [gather_pieces(sizes, order[0], held[n]) for n, order in enumerate(orders)]
        swapped = [[lax.ppermute(pieces[0], "dp", swap)] if paired else [] for pieces in halves]

        total = jnp.concatenate(
            [added(kept[n], received[n]).astype(jnp.bfloat16) for n in range(2)], axis=1
        )
        chunks = split(total, sizes[0])
        normed_grad = added(chunks[0], sent(chunks, sizes, 0))
        input_grad = norm_backward(scaled, inverse, normed_grad, norm_gain, stream_grad)

        if paired:
            halves = [
                pieces + near + [lax.ppermute(piece, "dp", swap) for piece in pieces[1:]]
                for pieces, near in zip(halves, swapped)
            ]
        weight_grad = weight_product(halves, grads)
        if groups > 1 and not paired:
            weight_grad = lax.psum(weight_grad, "dp")
        return (input_grad, weight_grad)

    return shards


def solution(mesh):
    placed = (
        P(("dp", "tensor"), None),
        P(),
        P(),
        P("dp", "tensor"),
        P(("dp", "tensor"), None),
        P(None, "tensor"),
    )
    return jax.shard_map(
        program(sizes_of(mesh.shape["tensor"]), mesh.shape["dp"]),
        mesh=mesh,
        in_specs=placed,
        out_specs=(P(("dp", "tensor"), None), P(None, "tensor")),
        check_vma=False,
    )
```

```python
import jax
import jax.numpy as jnp
from jax import lax
from jax.experimental import pallas as pl
from jax.sharding import PartitionSpec as P


epsilon = 1e-05


def sizes_of(count):
    outer = 4 if count % 4 == 0 else 1
    rest = count // outer
    inner = 2 if rest % 2 == 0 else 1
    return (outer, rest // inner, inner)


def moved(sizes, axis, step):
    outer, middle, inner = sizes
    pairs = []
    for index in range(outer * middle * inner):
        place = [index // (middle * inner), index // inner % middle, index % inner]
        place[axis] = (place[axis] + step) % sizes[axis]
        pairs.append((index, (place[0] * middle + place[1]) * inner + place[2]))
    return pairs


def gather_pieces(sizes, axis, values):
    return [values] + [
        lax.ppermute(values, "tensor", moved(sizes, axis, -step)) for step in range(1, sizes[axis])
    ]


def row_selector(sizes, order, rows):
    index = lax.axis_index("tensor")
    outer, middle, inner = sizes
    own = [index // (middle * inner), index // inner % middle, index % inner]
    count = outer * middle * inner
    tokens = rows // count
    row = lax.broadcasted_iota(jnp.int32, (rows, rows), 0)
    column = lax.broadcasted_iota(jnp.int32, (rows, rows), 1)
    left = row // tokens
    places = [None, None, None]
    for axis in reversed(order):
        places[axis] = (left % sizes[axis] + own[axis]) % sizes[axis]
        left = left // sizes[axis]
    source = ((places[0] * middle + places[1]) * inner + places[2]) * tokens + row % tokens
    return (source == column).astype(jnp.bfloat16)


def picked(selector, values):
    return lax.dot_general(
        selector, values, (((1,), (0,)), ((), ())), preferred_element_type=jnp.float32
    ).astype(jnp.bfloat16)


def weight_kernel(counts, steps_each):
    def body(*refs):
        out_ref = refs[-1]
        step = pl.program_id(0)
        start = 0
        for number, count in enumerate(counts):
            piece_refs = refs[start : start + count]
            grad_ref = refs[start + count]
            start += count + 1

            @pl.when(step // steps_each == number)
            def _():
                tall = jnp.concatenate([ref[...] for ref in piece_refs], axis=0)
                out_ref[...] = lax.dot_general(
                    tall, grad_ref[...], (((0,), (0,)), ((), ())), preferred_element_type=jnp.float32
                ).astype(out_ref.dtype)

    return body


def weight_product(segments, grads, firsts, height, base):
    width = segments[0][0].shape[1]
    block = next(size for size in (512, 256, 128) if width % size == 0)
    steps_each = width // block
    features = grads[0].shape[1]
    places = [first // block for first in firsts]
    specs, operands = [], []
    for number, (pieces, grad) in enumerate(zip(segments, grads)):
        for piece in pieces:
            specs.append(
                pl.BlockSpec(
                    (piece.shape[0], block),
                    lambda i, n=number: (0, jnp.clip(i - n * steps_each, 0, steps_each - 1)),
                )
            )
            operands.append(piece)
        specs.append(pl.BlockSpec(grad.shape, lambda i: (0, 0)))
        operands.append(grad)
    aliases = {}
    if base is not None:
        aliases = {len(operands): 0}
        specs.append(pl.BlockSpec(memory_space=pl.ANY))
        operands.append(base)
    rows = grads[0].shape[0]

    def out_at(i):
        return (jnp.where(i < steps_each, places[0] + i, places[1] + i - steps_each), 0)

    return pl.pallas_call(
        weight_kernel([len(pieces) for pieces in segments], steps_each),
        grid=(2 * steps_each,),
        in_specs=specs,
        out_specs=pl.BlockSpec((block, features), out_at),
        out_shape=jax.ShapeDtypeStruct((height, features), jnp.bfloat16),
        input_output_aliases=aliases,
        cost_estimate=pl.CostEstimate(
            flops=4 * rows * width * features, transcendentals=0, bytes_accessed=4 * width * features
        ),
        name="weight_product",
    )(*operands)


def after(value, *others):
    return lax.optimization_barrier((value,) + others)[0]


def normalize(values, norm_gain, norm_bias):
    as_float = values.astype(jnp.float32)
    centre = jnp.mean(as_float, axis=-1, keepdims=True)
    offsets = as_float - centre
    variance = jnp.mean(offsets * offsets, axis=-1, keepdims=True)
    inverse = lax.rsqrt(variance + epsilon)
    scaled = offsets * inverse
    normed = (scaled * norm_gain + norm_bias).astype(jnp.bfloat16)
    return (scaled, inverse, normed)


def norm_backward(scaled, inverse, normed_grad, norm_gain, stream_grad):
    weighted = normed_grad * norm_gain
    first_moment = jnp.mean(weighted, axis=-1, keepdims=True)
    second_moment = jnp.mean(weighted * scaled, axis=-1, keepdims=True)
    result = stream_grad.astype(jnp.float32) + inverse * (
        weighted - first_moment - scaled * second_moment
    )
    return result.astype(jnp.bfloat16)


def split(values, count):
    tall = values.shape[0] // count
    return [values[step * tall : (step + 1) * tall] for step in range(count)]


def sent(chunks, sizes, axis):
    return [
        lax.ppermute(chunks[step], "tensor", moved(sizes, axis, step))
        for step in range(1, sizes[axis])
    ]


def added(own, received):
    total = own.astype(jnp.float32)
    for values in received:
        total = total + values.astype(jnp.float32)
    return total


def contracted(grad, weight_rows):
    return lax.dot_general(
        grad, weight_rows, (((1,), (1,)), ((), ())), preferred_element_type=jnp.float32
    ).astype(jnp.bfloat16)


def program(sizes, groups):
    orders = ((2, 1, 0), (1, 2, 0))

    def layer(inputs, norm_gain, norm_bias, query_grad, stream_grad, query_weight):
        width = inputs.shape[1] // 2
        rows = query_grad.shape[0]
        paired = groups == 2
        swap = [(0, 1), (1, 0)]

        selectors = [row_selector(sizes, order, rows) for order in orders]
        grads = [picked(selector, query_grad) for selector in selectors]
        weights = [query_weight[:width], query_weight[width:]]

        tops = [split(grads[n], sizes[order[0]]) for n, order in enumerate(orders)]
        going = [[contracted(g, weights[n]) for g in tops[n][1:]] for n in range(2)]
        leaving = [sent([None] + going[n], sizes, order[0]) for n, order in enumerate(orders)]

        inputs = after(inputs, *going[0], *going[1])
        scaled, inverse, normed = normalize(inputs, norm_gain, norm_bias)
        normed = after(normed)
        outer_pieces = gather_pieces(sizes, 0, normed)
        top0, top1, query_grad = lax.optimization_barrier(
            (tops[0][0], tops[1][0], query_grad, normed)
        )[:3]
        kept = [contracted(top0, weights[0]), contracted(top1, weights[1])]
        if paired:
            other_grad = lax.ppermute(query_grad, "dp", swap)
            other = [picked(selector, other_grad) for selector in selectors]
            grads = [jnp.concatenate(pair, axis=0) for pair in zip(grads, other)]
        kept = list(lax.optimization_barrier((*kept, *grads))[:2])

        totals = [added(kept[n], leaving[n]).astype(jnp.bfloat16) for n in range(2)]
        chunks = [split(totals[n], sizes[order[1]]) for n, order in enumerate(orders)]
        received = [sent(chunks[n], sizes, order[1]) for n, order in enumerate(orders)]

        outer_pieces = list(lax.optimization_barrier((*outer_pieces, *totals))[: sizes[0]])
        held = [
            jnp.concatenate(
                [piece[:, number * width : (number + 1) * width] for piece in outer_pieces], axis=0
            )
            for number in range(2)
        ]
        second = [gather_pieces(sizes, order[1], held[n]) for n, order in enumerate(orders)]

        kept = [chunk[0] for chunk in chunks]
        kept = list(lax.optimization_barrier((*kept, *held))[:2])
        total = jnp.concatenate(
            [added(kept[n], received[n]).astype(jnp.bfloat16) for n in range(2)], axis=1
        )
        chunks = split(total, sizes[0])
        normed_grad = added(chunks[0], sent(chunks, sizes, 0))
        input_grad = norm_backward(scaled, inverse, normed_grad, norm_gain, stream_grad)

        parts = 2 if width % 256 == 0 else 1
        wide = width // parts
        flat = [piece for pieces in second for piece in pieces]
        flat = list(lax.optimization_barrier((*flat, total))[: len(flat)])
        second = [flat[: len(second[0])], flat[len(second[0]) :]]
        segments = []
        for part in range(parts):
            at = slice(part * wide, (part + 1) * wide)
            held = [jnp.concatenate([p[:, at] for p in pieces], axis=0) for pieces in second]
            segments.append(
                [gather_pieces(sizes, order[0], held[n]) for n, order in enumerate(orders)]
            )
        weight_grad = None
        for part in range(parts):
            pieces = segments[part]
            if weight_grad is not None:
                late = [piece for own in pieces for piece in own[1:]]
                late = lax.optimization_barrier((*late, weight_grad))
                weight_grad, late = late[-1], list(late[:-1])
                pieces = [[own[0]] + [late.pop(0) for _ in own[1:]] for own in pieces]
            if paired:
                pieces = [own + [lax.ppermute(p, "dp", swap) for p in own] for own in pieces]
            weight_grad = weight_product(
                pieces, grads, (part * wide, width + part * wide), 2 * width, weight_grad
            )
        if groups > 1 and not paired:
            weight_grad = lax.psum(weight_grad, "dp")
        return (input_grad, weight_grad)

    return layer


def solution(mesh):
    placed = (
        P(("dp", "tensor"), None),
        P(),
        P(),
        P("dp", "tensor"),
        P(("dp", "tensor"), None),
        P(None, "tensor"),
    )
    return jax.shard_map(
        program(sizes_of(mesh.shape["tensor"]), mesh.shape["dp"]),
        mesh=mesh,
        in_specs=placed,
        out_specs=(P(("dp", "tensor"), None), P(None, "tensor")),
        check_vma=False,
    )
```

```python
import jax
import jax.numpy as jnp
from jax import lax
from jax.experimental import pallas as pl
from jax.sharding import PartitionSpec as P


epsilon = 1e-05


def sizes_of(count):
    outer = 4 if count % 4 == 0 else 1
    rest = count // outer
    inner = 2 if rest % 2 == 0 else 1
    return (outer, rest // inner, inner)


def moved(sizes, axis, step):
    outer, middle, inner = sizes
    pairs = []
    for index in range(outer * middle * inner):
        place = [index // (middle * inner), index // inner % middle, index % inner]
        place[axis] = (place[axis] + step) % sizes[axis]
        pairs.append((index, (place[0] * middle + place[1]) * inner + place[2]))
    return pairs


def gather_pieces(sizes, axis, values):
    return [values] + [
        lax.ppermute(values, "tensor", moved(sizes, axis, -step)) for step in range(1, sizes[axis])
    ]


def row_selector(sizes, order, rows):
    index = lax.axis_index("tensor")
    outer, middle, inner = sizes
    own = [index // (middle * inner), index // inner % middle, index % inner]
    count = outer * middle * inner
    tokens = rows // count
    row = lax.broadcasted_iota(jnp.int32, (rows, rows), 0)
    column = lax.broadcasted_iota(jnp.int32, (rows, rows), 1)
    left = row // tokens
    places = [None, None, None]
    for axis in reversed(order):
        places[axis] = (left % sizes[axis] + own[axis]) % sizes[axis]
        left = left // sizes[axis]
    source = ((places[0] * middle + places[1]) * inner + places[2]) * tokens + row % tokens
    return (source == column).astype(jnp.bfloat16)


def picked(selector, values):
    return lax.dot_general(
        selector, values, (((1,), (0,)), ((), ())), preferred_element_type=jnp.float32
    ).astype(jnp.bfloat16)


def weight_kernel(counts, steps_each):
    def body(*refs):
        out_ref = refs[-1]
        step = pl.program_id(0)
        start = 0
        for number, count in enumerate(counts):
            piece_refs = refs[start : start + count]
            grad_ref = refs[start + count]
            start += count + 1

            @pl.when(step // steps_each == number)
            def _():
                tall = jnp.concatenate([ref[...] for ref in piece_refs], axis=0)
                out_ref[...] = lax.dot_general(
                    tall, grad_ref[...], (((0,), (0,)), ((), ())), preferred_element_type=jnp.float32
                ).astype(out_ref.dtype)

    return body


def weight_product(segments, grads, firsts, height, base):
    width = segments[0][0].shape[1]
    block = next(size for size in (512, 256, 128) if width % size == 0)
    steps_each = width // block
    features = grads[0].shape[1]
    places = [first // block for first in firsts]
    specs, operands = [], []
    for number, (pieces, grad) in enumerate(zip(segments, grads)):
        for piece in pieces:
            specs.append(
                pl.BlockSpec(
                    (piece.shape[0], block),
                    lambda i, n=number: (0, jnp.clip(i - n * steps_each, 0, steps_each - 1)),
                )
            )
            operands.append(piece)
        specs.append(pl.BlockSpec(grad.shape, lambda i: (0, 0)))
        operands.append(grad)
    aliases = {}
    if base is not None:
        aliases = {len(operands): 0}
        specs.append(pl.BlockSpec(memory_space=pl.ANY))
        operands.append(base)
    rows = grads[0].shape[0]

    def out_at(i):
        return (jnp.where(i < steps_each, places[0] + i, places[1] + i - steps_each), 0)

    return pl.pallas_call(
        weight_kernel([len(pieces) for pieces in segments], steps_each),
        grid=(2 * steps_each,),
        in_specs=specs,
        out_specs=pl.BlockSpec((block, features), out_at),
        out_shape=jax.ShapeDtypeStruct((height, features), jnp.bfloat16),
        input_output_aliases=aliases,
        cost_estimate=pl.CostEstimate(
            flops=4 * rows * width * features, transcendentals=0, bytes_accessed=4 * width * features
        ),
        name="weight_product",
    )(*operands)


def after(value, *others):
    return lax.optimization_barrier((value,) + others)[0]


def normalize(values, norm_gain, norm_bias):
    as_float = values.astype(jnp.float32)
    centre = jnp.mean(as_float, axis=-1, keepdims=True)
    offsets = as_float - centre
    variance = jnp.mean(offsets * offsets, axis=-1, keepdims=True)
    inverse = lax.rsqrt(variance + epsilon)
    scaled = offsets * inverse
    normed = (scaled * norm_gain + norm_bias).astype(jnp.bfloat16)
    return (scaled, inverse, normed)


def norm_backward(scaled, inverse, normed_grad, norm_gain, stream_grad):
    weighted = normed_grad * norm_gain
    first_moment = jnp.mean(weighted, axis=-1, keepdims=True)
    second_moment = jnp.mean(weighted * scaled, axis=-1, keepdims=True)
    result = stream_grad.astype(jnp.float32) + inverse * (
        weighted - first_moment - scaled * second_moment
    )
    return result.astype(jnp.bfloat16)


def split(values, count):
    tall = values.shape[0] // count
    return [values[step * tall : (step + 1) * tall] for step in range(count)]


def sent(chunks, sizes, axis):
    return [
        lax.ppermute(chunks[step], "tensor", moved(sizes, axis, step))
        for step in range(1, sizes[axis])
    ]


def added(own, received):
    total = own.astype(jnp.float32)
    for values in received:
        total = total + values.astype(jnp.float32)
    return total


def contracted(grad, weight_rows):
    return lax.dot_general(
        grad, weight_rows, (((1,), (1,)), ((), ())), preferred_element_type=jnp.float32
    ).astype(jnp.bfloat16)


def program(sizes, groups):
    orders = ((2, 1, 0), (1, 2, 0))

    def layer(inputs, norm_gain, norm_bias, query_grad, stream_grad, query_weight):
        width = inputs.shape[1] // 2
        rows = query_grad.shape[0]
        paired = groups == 2
        swap = [(0, 1), (1, 0)]

        selectors = [row_selector(sizes, order, rows) for order in orders]
        grads = [picked(selector, query_grad) for selector in selectors]
        weights = [query_weight[:width], query_weight[width:]]

        tops = [split(grads[n], sizes[order[0]]) for n, order in enumerate(orders)]
        going = [[contracted(g, weights[n]) for g in tops[n][1:]] for n in range(2)]
        leaving = [sent([None] + going[n], sizes, order[0]) for n, order in enumerate(orders)]

        inputs = after(inputs, *going[0], *going[1])
        scaled, inverse, normed = normalize(inputs, norm_gain, norm_bias)
        normed = after(normed)
        outer_pieces = gather_pieces(sizes, 0, normed)
        top0, top1, query_grad = lax.optimization_barrier(
            (tops[0][0], tops[1][0], query_grad, normed)
        )[:3]
        kept = [contracted(top0, weights[0]), contracted(top1, weights[1])]
        if paired:
            other_grad = lax.ppermute(query_grad, "dp", swap)
            other = [picked(selector, other_grad) for selector in selectors]
            grads = [jnp.concatenate(pair, axis=0) for pair in zip(grads, other)]
        kept = list(lax.optimization_barrier((*kept, *grads))[:2])

        totals = [added(kept[n], leaving[n]).astype(jnp.bfloat16) for n in range(2)]
        chunks = [split(totals[n], sizes[order[1]]) for n, order in enumerate(orders)]
        received = [sent(chunks[n], sizes, order[1]) for n, order in enumerate(orders)]

        outer_pieces = list(lax.optimization_barrier((*outer_pieces, *totals))[: sizes[0]])
        held = [
            jnp.concatenate(
                [piece[:, number * width : (number + 1) * width] for piece in outer_pieces], axis=0
            )
            for number in range(2)
        ]
        second = [gather_pieces(sizes, order[1], held[n]) for n, order in enumerate(orders)]

        kept = [chunk[0] for chunk in chunks]
        kept = list(lax.optimization_barrier((*kept, *held))[:2])
        total = jnp.concatenate(
            [added(kept[n], received[n]).astype(jnp.bfloat16) for n in range(2)], axis=1
        )
        chunks = split(total, sizes[0])
        third = sent(chunks, sizes, 0)

        parts = 2 if width % 256 == 0 else 1
        wide = width // parts
        flat = [piece for pieces in second for piece in pieces]
        flat = list(lax.optimization_barrier((*flat, total))[: len(flat)])
        second = [flat[: len(second[0])], flat[len(second[0]) :]]
        segments = []
        for part in range(parts):
            at = slice(part * wide, (part + 1) * wide)
            held = [jnp.concatenate([p[:, at] for p in pieces], axis=0) for pieces in second]
            segments.append(
                [gather_pieces(sizes, order[0], held[n]) for n, order in enumerate(orders)]
            )
        weight_grad = None
        for part in range(parts):
            pieces = segments[part]
            if weight_grad is not None:
                late = [piece for own in pieces for piece in own[1:]]
                late = lax.optimization_barrier((*late, *third, weight_grad))
                weight_grad, third, late = late[-1], late[-sizes[0] : -1], list(late[: -sizes[0]])
                pieces = [[own[0]] + [late.pop(0) for _ in own[1:]] for own in pieces]
            if paired:
                pieces = [own + [lax.ppermute(p, "dp", swap) for p in own] for own in pieces]
            weight_grad = weight_product(
                pieces, grads, (part * wide, width + part * wide), 2 * width, weight_grad
            )
        normed_grad = added(chunks[0], third)
        input_grad = norm_backward(scaled, inverse, normed_grad, norm_gain, stream_grad)
        if groups > 1 and not paired:
            weight_grad = lax.psum(weight_grad, "dp")
        return (input_grad, weight_grad)

    return layer


def solution(mesh):
    placed = (
        P(("dp", "tensor"), None),
        P(),
        P(),
        P("dp", "tensor"),
        P(("dp", "tensor"), None),
        P(None, "tensor"),
    )
    return jax.shard_map(
        program(sizes_of(mesh.shape["tensor"]), mesh.shape["dp"]),
        mesh=mesh,
        in_specs=placed,
        out_specs=(P(("dp", "tensor"), None), P(None, "tensor")),
        check_vma=False,
    )
```
